32 devices in a mesh: row: 2 (over x), col: 4 (over y, core), layer: 4 (over z).
Axes of the slice: x: 2, y: 2, z: 4, core: 2. Of those that a mesh axis runs over, the one named last changes fastest.
Arguments:
- panel: float32 [1024, 8192], P('layer', ('col', 'row')), may hold values from -0.75 to 0.75
- c_in: float32 [4, 2, 1024, 8192], P('layer', 'row', None, 'col'), may hold values from -1.5 to 1.5
Outputs:
- updated: float32 [4, 2, 1024, 8192], P('layer', 'row', None, 'col')
The draws below stay inside these ranges and needn't reach their ends.
All inputs are finite; a program needn't handle non-finite values.
Results may differ from the reference program's by a relative error of at most 0.000062.
Values sent between devices are 32-bit elements; how exact they have to be, the bound alone decides.
A program may use at most 128 MiB of HBM per device.

```python
import jax
import jax.numpy as jnp
from jax import lax

N = 8192
K = 1024
W = 1024
N_ROW = 2
N_COL = 4


def steps_of(stream_key, extent, pieces, smallest, largest):
    level = 1.0
    for position, parts in pieces:
        draws = jax.random.uniform(jax.random.fold_in(jax.random.fold_in(stream_key, 6), position), (parts,), jnp.float32, smallest / len(pieces), largest / len(pieces))
        level = level * jnp.repeat(jnp.exp(draws), extent[position] // parts).reshape((-1,) + (1,) * (len(extent) - 1 - position))
    return level


def noise(key, shape, spread, limit, shards=(), held_as=jnp.bfloat16):
    values = spread * jax.random.normal(key, shape, jnp.float32)
    if shards:
        values = values * steps_of(key, shape, shards, -0.22, 0.18)
    return jnp.clip(values, -limit, limit).astype(held_as)


def setup_inputs(seed: int = 0) -> dict:
    arg_keys = jax.random.split(jax.random.key(seed), 3)
    return {
        "panel": noise(arg_keys[0], (K, N), (0.3 * K ** -0.25), 0.75, ((0, 4), (1, 8)), jnp.float32),
        "c_in": noise(arg_keys[1], (N_COL, N_ROW, W, N), 0.1, 1.5, ((0, 4), (1, 2), (3, 4)), jnp.float32),
    }


def reference(panel, c_in):
    gram = lax.dot_general(panel, panel, (((0,), (0,)), ((), ())), precision=lax.Precision.HIGHEST, preferred_element_type=jnp.float32)
    gram = gram.reshape(N_COL, N_ROW, N // (N_ROW * N_COL), N)
    return c_in + gram
```

```python
import functools

import jax
import jax.numpy as jnp
from jax import lax
from jax.experimental import pallas as pl
from jax.experimental.pallas import tpu as pltpu
from jax.sharding import PartitionSpec as P

MESH = pl.DeviceIdType.MESH


def product(left, right):
    return lax.dot_general(
        left,
        right,
        (((0,), (0,)), ((), ())),
        precision=lax.Precision.HIGHEST,
        preferred_element_type=jnp.float32,
    )


def general(panel, c_in):
    narrow = c_in.shape[2]
    spread = lax.all_gather(panel, "col", axis=1, tiled=True)
    local = lax.all_gather(panel, "row", axis=1, tiled=True)
    groups = spread.shape[1] // narrow
    tile = product(spread, local)
    tile = tile.reshape(groups, 1, narrow, local.shape[1])
    summed = lax.psum_scatter(tile, "layer", scatter_dimension=0, tiled=True)
    return c_in + summed


def gather_and_update(
    panel, c_in, out, cols, rows, left3, own_sem, c_sem,
    got, row_got, to_x, to_in, to_out, to_partner, to_far,
):
    x = lax.axis_index("row")
    c = lax.axis_index("col")
    z = lax.axis_index("layer")
    depth, narrow = panel.shape
    half = depth // 2
    flip = z // 2
    lane = c % 2
    inward = z + 1 - 2 * flip
    outward = z - 1 + 2 * flip
    at_end = (z == 0) | (z == 3)
    partner = c + 1 - 2 * lane
    far = 2 * (1 - flip)
    is_owner = c == z
    is_far = (c // 2) != flip
    same, other = x, 1 - x

    def layer(k):
        return k + flip * (3 - 2 * k)

    def part(h):
        return pl.ds(pl.multiple_of(h * half, half), half)

    def remote(src, dst, send_sem, recv_sem, **device):
        return pltpu.make_async_remote_copy(
            src_ref=src, dst_ref=dst, send_sem=send_sem, recv_sem=recv_sem,
            device_id=device, device_id_type=MESH,
        )

    def chunk_copy(b, k, h, sems, **device):
        ref = cols.at[b, layer(k), part(h)]
        return remote(ref, ref, sems.at[b, layer(k), h], got.at[b, layer(k), h], **device)

    def arrived(b, k, h):
        chunk_copy(b, k, h, to_x, row=1 - x).wait_recv()

    def row_arrived(k, h):
        ref = rows.at[layer(k), part(h)]
        remote(ref, ref, to_partner.at[layer(k), h], row_got.at[layer(k), h], col=partner).wait_recv()

    def owner_copies(k, h):
        src = cols.at[same, layer(k), part(h)]
        dst = rows.at[layer(k), part(h)]
        return (
            remote(src, dst, to_far.at[layer(k), h], row_got.at[layer(k), h], col=far + h),
            remote(src, dst, to_partner.at[layer(k), h], row_got.at[layer(k), h], col=partner),
        )

    def far_copy(k):
        ref = rows.at[layer(k), part(lane)]
        return remote(ref, ref, to_partner.at[layer(k), lane], row_got.at[layer(k), lane], col=partner)

    def share_rows(k, h):
        @pl.when(is_owner)
        def _():
            for copy in owner_copies(k, h):
                copy.start()

    def prepare(k):
        @pl.when(is_far)
        def _():
            row_arrived(k, lane)
            far_copy(k).start()
            row_arrived(k, 1 - lane)

        @pl.when(jnp.logical_not(is_far) & jnp.logical_not(is_owner))
        def _():
            row_arrived(k, 0)
            row_arrived(k, 1)

        def split(load):
            def body(i, carry):
                span = pl.ds(pl.multiple_of(i * 256, 256), 256)
                block = load(span).T
                high = block.astype(jnp.bfloat16)
                low = (block - high.astype(jnp.float32)).astype(jnp.bfloat16)
                left3[span, 0:depth] = high
                left3[span, depth : 2 * depth] = high
                left3[span, 2 * depth : 3 * depth] = low
                return carry

            lax.fori_loop(0, narrow // 256, body, 0)

        @pl.when(is_owner)
        def _():
            split(lambda span: cols[same, layer(k), :, span])

        @pl.when(jnp.logical_not(is_owner))
        def _():
            split(lambda span: rows[layer(k), :, span])

    def multiply(b, k):
        def body(i, carry):
            span = pl.ds(pl.multiple_of(i * 256, 256), 256)
            wide = pl.ds(pl.multiple_of(b * narrow + i * 256, 256), 256)
            block = cols[b, layer(k), :, span]
            high = block.astype(jnp.bfloat16)
            low = (block - high.astype(jnp.float32)).astype(jnp.bfloat16)
            right3 = jnp.concatenate([high, low, high], axis=0)
            for m in range(0, narrow, 512):
                out[m : m + 512, wide] += jnp.dot(
                    left3[m : m + 512, :], right3, preferred_element_type=jnp.float32
                )
            return carry

        lax.fori_loop(0, narrow // 256, body, 0)

    own = pltpu.make_async_copy(panel, cols.at[same, z], own_sem)
    own.start()
    base = pltpu.make_async_copy(c_in, out, c_sem)
    base.start()

    barrier = pltpu.get_barrier_semaphore()

    def greet(**device):
        pl.semaphore_signal(barrier, inc=1, device_id=device, device_id_type=MESH)

    greet(row=1 - x)
    greet(layer=inward)
    for step in range(1, 4):
        greet(col=(c + step) % 4)

    @pl.when(jnp.logical_not(at_end))
    def _():
        greet(layer=outward)

    pl.semaphore_wait(barrier, jnp.where(at_end, 5, 6))
    own.wait()

    @pl.when(at_end)
    def _():
        sent = []

        def send(b, k, h, sems, **device):
            copy = chunk_copy(b, k, h, sems, **device)
            copy.start()
            sent.append(copy)

        for h in range(2):
            send(same, 0, h, to_in, layer=inward)
            send(same, 0, h, to_x, row=1 - x)
            share_rows(0, h)
        for h in range(2):
            arrived(same, 1, h)
            send(same, 1, h, to_x, row=1 - x)
            share_rows(1, h)
            arrived(other, 0, h)
            send(other, 0, h, to_in, layer=inward)
        base.wait()
        prepare(0)
        multiply(same, 0)
        multiply(other, 0)
        arrived(same, 2, 0)
        send(same, 2, 0, to_x, row=1 - x)
        share_rows(2, 0)
        prepare(1)
        multiply(same, 1)
        arrived(same, 2, 1)
        send(same, 2, 1, to_x, row=1 - x)
        share_rows(2, 1)
        arrived(other, 1, 0)
        arrived(other, 1, 1)
        multiply(other, 1)
        arrived(same, 3, 0)
        send(same, 3, 0, to_x, row=1 - x)
        share_rows(3, 0)
        prepare(2)
        multiply(same, 2)
        arrived(same, 3, 1)
        share_rows(3, 1)
        arrived(other, 2, 0)
        arrived(other, 2, 1)
        multiply(other, 2)
        prepare(3)
        multiply(same, 3)
        arrived(other, 3, 0)
        arrived(other, 3, 1)
        multiply(other, 3)
        for copy in sent:
            copy.wait_send()

    @pl.when(jnp.logical_not(at_end))
    def _():
        sent = []

        def send(b, k, h, sems, **device):
            copy = chunk_copy(b, k, h, sems, **device)
            copy.start()
            sent.append(copy)

        for h in range(2):
            send(same, 1, h, to_out, layer=outward)
            send(same, 1, h, to_in, layer=inward)
            send(same, 1, h, to_x, row=1 - x)
            share_rows(1, h)
        for h in range(2):
            arrived(same, 2, h)
            send(same, 2, h, to_out, layer=outward)
            send(same, 2, h, to_x, row=1 - x)
            share_rows(2, h)
            arrived(same, 0, h)
            send(same, 0, h, to_in, layer=inward)
            share_rows(0, h)
        base.wait()
        prepare(1)
        multiply(same, 1)
        arrived(other, 1, 0)
        arrived(other, 1, 1)
        multiply(other, 1)
        for h in range(2):
            arrived(same, 3, h)
            send(same, 3, h, to_out, layer=outward)
            send(same, 3, h, to_x, row=1 - x)
            share_rows(3, h)
        prepare(0)
        multiply(same, 0)
        arrived(other, 0, 0)
        arrived(other, 0, 1)
        multiply(other, 0)
        prepare(2)
        multiply(same, 2)
        arrived(other, 2, 0)
        arrived(other, 2, 1)
        arrived(other, 3, 0)
        arrived(other, 3, 1)
        send(other, 3, 1, to_out, layer=outward)
        multiply(other, 2)
        prepare(3)
        multiply(same, 3)
        multiply(other, 3)
        for copy in sent:
            copy.wait_send()

    @pl.when(is_owner)
    def _():
        for k in range(4):
            for h in range(2):
                for copy in owner_copies(k, h):
                    copy.wait_send()

    @pl.when(is_far)
    def _():
        for k in range(4):
            far_copy(k).wait_send()


def lined_up(panel, c_in):
    depth, narrow = panel.shape
    wide = c_in.shape[3]
    dma = pltpu.SemaphoreType.DMA
    updated = pl.pallas_call(
        gather_and_update,
        out_shape=pltpu.VMEM((narrow, wide), jnp.float32),
        in_specs=[pl.BlockSpec(memory_space=pl.ANY)] * 2,
        out_specs=pl.BlockSpec(memory_space=pltpu.VMEM),
        scratch_shapes=[
            pltpu.VMEM((2, 4, depth, narrow), jnp.float32),
            pltpu.VMEM((4, depth, narrow), jnp.float32),
            pltpu.VMEM((narrow, 3 * depth), jnp.bfloat16),
            dma, dma,
            dma((2, 4, 2)),
            dma((4, 2)),
            dma((2, 4, 2)),
            dma((2, 4, 2)),
            dma((2, 4, 2)),
            dma((4, 2)),
            dma((4, 2)),
        ],
        compiler_params=pltpu.CompilerParams(
            collective_id=0, has_side_effects=True, vmem_limit_bytes=48 << 20
        ),
    )(panel, c_in.reshape(narrow, wide))
    return updated.reshape(c_in.shape)


def on_device(sizes, panel, c_in):
    depth, narrow = panel.shape
    fits = (
        sizes == (2, 4, 4)
        and c_in.shape == (1, 1, narrow, 2 * narrow)
        and narrow % 512 == 0
        and depth % 256 == 0
    )
    return (lined_up if fits else general)(panel, c_in)


def solution(mesh):
    sizes = tuple(mesh.shape[name] for name in ("row", "col", "layer"))
    return jax.shard_map(
        functools.partial(on_device, sizes),
        mesh=mesh,
        in_specs=(P("layer", ("col", "row")), P("layer", "row", None, "col")),
        out_specs=P("layer", "row", None, "col"),
        check_vma=False,
    )
```

```python
import functools

import jax
import jax.numpy as jnp
from jax import lax
from jax.experimental import pallas as pl
from jax.experimental.pallas import tpu as pltpu
from jax.sharding import PartitionSpec as P

MESH = pl.DeviceIdType.MESH


def product(left, right):
    return lax.dot_general(
        left,
        right,
        (((0,), (0,)), ((), ())),
        precision=lax.Precision.HIGHEST,
        preferred_element_type=jnp.float32,
    )


def general(panel, c_in):
    narrow = c_in.shape[2]
    spread = lax.all_gather(panel, "col", axis=1, tiled=True)
    local = lax.all_gather(panel, "row", axis=1, tiled=True)
    groups = spread.shape[1] // narrow
    tile = product(spread, local)
    tile = tile.reshape(groups, 1, narrow, local.shape[1])
    summed = lax.psum_scatter(tile, "layer", scatter_dimension=0, tiled=True)
    return c_in + summed


def gather_and_update(
    panel, c_in, out, cols, rows, left3, own_sem, c_sem,
    got, row_got, to_x, to_in, to_out, to_partner, to_far,
):
    x = lax.axis_index("row")
    c = lax.axis_index("col")
    z = lax.axis_index("layer")
    depth, narrow = panel.shape
    width = narrow // 4
    flip = z // 2
    lane = c % 2
    inward = z + 1 - 2 * flip
    outward = z - 1 + 2 * flip
    at_end = (z == 0) | (z == 3)
    partner = c + 1 - 2 * lane
    far = 2 * (1 - flip)
    is_owner = c == z
    is_far = (c // 2) != flip
    same, other = x, 1 - x

    def layer(k):
        return k + flip * (3 - 2 * k)

    def part(h):
        return pl.ds(pl.multiple_of(h * width, width), width)

    def remote(src, dst, send_sem, recv_sem, **device):
        return pltpu.make_async_remote_copy(
            src_ref=src, dst_ref=dst, send_sem=send_sem, recv_sem=recv_sem,
            device_id=device, device_id_type=MESH,
        )

    def chunk_copy(b, k, h, sems, **device):
        ref = cols.at[b, layer(k), :, part(h)]
        return remote(ref, ref, sems.at[b, layer(k), h], got.at[b, layer(k), h], **device)

    def arrived(b, k, h):
        chunk_copy(b, k, h, to_x, row=1 - x).wait_recv()

    def row_arrived(k, h):
        ref = rows.at[layer(k), :, part(h)]
        remote(ref, ref, to_partner.at[layer(k), h], row_got.at[layer(k), h], col=partner).wait_recv()

    def owner_copies(k, h):
        src = cols.at[same, layer(k), :, part(h)]
        dst = rows.at[layer(k), :, part(h)]
        return (
            remote(src, dst, to_far.at[layer(k), h], row_got.at[layer(k), h], col=far + h % 2),
            remote(src, dst, to_partner.at[layer(k), h], row_got.at[layer(k), h], col=partner),
        )

    def far_copy(k, h):
        ref = rows.at[layer(k), :, part(h)]
        return remote(ref, ref, to_partner.at[layer(k), h], row_got.at[layer(k), h], col=partner)

    def share_rows(k, h):
        @pl.when(is_owner)
        def _():
            for copy in owner_copies(k, h):
                copy.start()

    def prepare(k):
        @pl.when(is_far)
        def _():
            for h in (lane, lane + 2):
                row_arrived(k, h)
                far_copy(k, h).start()
            for h in (1 - lane, 3 - lane):
                row_arrived(k, h)

        @pl.when(jnp.logical_not(is_far) & jnp.logical_not(is_owner))
        def _():
            for h in range(4):
                row_arrived(k, h)

        def split(load):
            def body(i, carry):
                span = part(i)
                block = load(span).T
                high = block.astype(jnp.bfloat16)
                low = (block - high.astype(jnp.float32)).astype(jnp.bfloat16)
                left3[span, 0:depth] = high
                left3[span, depth : 2 * depth] = high
                left3[span, 2 * depth : 3 * depth] = low
                return carry

            lax.fori_loop(0, 4, body, 0)

        @pl.when(is_owner)
        def _():
            split(lambda span: cols[same, layer(k), :, span])

        @pl.when(jnp.logical_not(is_owner))
        def _():
            split(lambda span: rows[layer(k), :, span])

    def multiply(b, k, first=0, step=1):
        def body(i, carry):
            span = part(first + i * step)
            wide = pl.ds(pl.multiple_of(b * narrow + (first + i * step) * width, width), width)
            block = cols[b, layer(k), :, span]
            high = block.astype(jnp.bfloat16)
            low = (block - high.astype(jnp.float32)).astype(jnp.bfloat16)
            right3 = jnp.concatenate([high, low, high], axis=0)
            for m in range(0, narrow, 512):
                out[m : m + 512, wide] += jnp.dot(
                    left3[m : m + 512, :], right3, preferred_element_type=jnp.float32
                )
            return carry

        lax.fori_loop(0, 4 // step, body, 0)

    own = pltpu.make_async_copy(panel, cols.at[same, z], own_sem)
    own.start()
    base = pltpu.make_async_copy(c_in, out, c_sem)
    base.start()

    barrier = pltpu.get_barrier_semaphore()

    def greet(**device):
        pl.semaphore_signal(barrier, inc=1, device_id=device, device_id_type=MESH)

    greet(row=1 - x)
    greet(layer=inward)
    for step in range(1, 4):
        greet(col=(c + step) % 4)

    @pl.when(jnp.logical_not(at_end))
    def _():
        greet(layer=outward)

    pl.semaphore_wait(barrier, jnp.where(at_end, 5, 6))
    own.wait()

    @pl.when(at_end)
    def _():
        sent = []

        def send(b, k, h, sems, **device):
            copy = chunk_copy(b, k, h, sems, **device)
            copy.start()
            sent.append(copy)

        def relay(k, h):
            arrived(same, k, h)
            send(same, k, h, to_x, row=1 - x)
            share_rows(k, h)

        for h in range(4):
            send(same, 0, h, to_in, layer=inward)
            send(same, 0, h, to_x, row=1 - x)
            share_rows(0, h)
        for h in range(4):
            arrived(same, 1, h)
            send(same, 1, h, to_x, row=1 - x)
            share_rows(1, h)
            arrived(other, 0, h)
            send(other, 0, h, to_in, layer=inward)
        base.wait()
        prepare(0)
        multiply(same, 0)
        multiply(other, 0)
        for h in (0, 1):
            relay(2, h)
        prepare(1)
        multiply(same, 1)
        for h in (2, 3):
            relay(2, h)
        for h in range(4):
            arrived(other, 1, h)
        multiply(other, 1)
        for h in (0, 1):
            relay(3, h)
        prepare(2)
        multiply(same, 2)
        for h in (2, 3):
            arrived(same, 3, h)
            share_rows(3, h)
        for h in range(4):
            arrived(other, 2, h)
        multiply(other, 2)
        prepare(3)
        multiply(same, 3)
        for first in (0, 1):
            arrived(other, 3, first)
            arrived(other, 3, first + 2)
            multiply(other, 3, first, 2)
        for copy in sent:
            copy.wait_send()

    @pl.when(jnp.logical_not(at_end))
    def _():
        sent = []

        def send(b, k, h, sems, **device):
            copy = chunk_copy(b, k, h, sems, **device)
            copy.start()
            sent.append(copy)

        for h in range(4):
            send(same, 1, h, to_out, layer=outward)
            send(same, 1, h, to_in, layer=inward)
            send(same, 1, h, to_x, row=1 - x)
            share_rows(1, h)
        for h in range(4):
            arrived(same, 2, h)
            send(same, 2, h, to_out, layer=outward)
            send(same, 2, h, to_x, row=1 - x)
            share_rows(2, h)
            arrived(same, 0, h)
            send(same, 0, h, to_in, layer=inward)
            share_rows(0, h)
        base.wait()
        prepare(1)
        multiply(same, 1)
        for h in range(4):
            arrived(other, 1, h)
        multiply(other, 1)
        for h in range(4):
            arrived(same, 3, h)
            send(same, 3, h, to_out, layer=outward)
            share_rows(3, h)
        for h in (2, 3, 0, 1):
            send(same, 3, h, to_x, row=1 - x)
        prepare(0)
        multiply(same, 0)
        for h in range(4):
            arrived(other, 0, h)
        multiply(other, 0)
        prepare(2)
        multiply(same, 2)
        for h in (2, 3):
            arrived(other, 3, h)
            send(other, 3, h, to_out, layer=outward)
        for h in range(4):
            arrived(other, 2, h)
        multiply(other, 2)
        prepare(3)
        multiply(same, 3)
        for h in (0, 1):
            arrived(other, 3, h)
        multiply(other, 3)
        for copy in sent:
            copy.wait_send()

    @pl.when(is_owner)
    def _():
        for k in range(4):
            for h in range(4):
                for copy in owner_copies(k, h):
                    copy.wait_send()

    @pl.when(is_far)
    def _():
        for k in range(4):
            for h in (lane, lane + 2):
                far_copy(k, h).wait_send()


def lined_up(panel, c_in):
    depth, narrow = panel.shape
    wide = c_in.shape[3]
    dma = pltpu.SemaphoreType.DMA
    updated = pl.pallas_call(
        gather_and_update,
        out_shape=pltpu.VMEM((narrow, wide), jnp.float32),
        in_specs=[pl.BlockSpec(memory_space=pl.ANY)] * 2,
        out_specs=pl.BlockSpec(memory_space=pltpu.VMEM),
        scratch_shapes=[
            pltpu.VMEM((2, 4, depth, narrow), jnp.float32),
            pltpu.VMEM((4, depth, narrow), jnp.float32),
            pltpu.VMEM((narrow, 3 * depth), jnp.bfloat16),
            dma, dma,
            dma((2, 4, 4)),
            dma((4, 4)),
            dma((2, 4, 4)),
            dma((2, 4, 4)),
            dma((2, 4, 4)),
            dma((4, 4)),
            dma((4, 4)),
        ],
        compiler_params=pltpu.CompilerParams(
            collective_id=0, has_side_effects=True, vmem_limit_bytes=48 << 20
        ),
    )(panel, c_in.reshape(narrow, wide))
    return updated.reshape(c_in.shape)


def on_device(sizes, panel, c_in):
    depth, narrow = panel.shape
    fits = (
        sizes == (2, 4, 4)
        and c_in.shape == (1, 1, narrow, 2 * narrow)
        and narrow % 512 == 0
        and depth % 256 == 0
    )
    return (lined_up if fits else general)(panel, c_in)


def solution(mesh):
    sizes = tuple(mesh.shape[name] for name in ("row", "col", "layer"))
    return jax.shard_map(
        functools.partial(on_device, sizes),
        mesh=mesh,
        in_specs=(P("layer", ("col", "row")), P("layer", "row", None, "col")),
        out_specs=P("layer", "row", None, "col"),
        check_vma=False,
    )
```
